32 devices in a mesh: slab: 4 (over z), sub: 8 (over y, x, core).
Axes of the slice: x: 2, y: 2, z: 4, core: 2. Of those that a mesh axis runs over, the one named last changes fastest.
Arguments:
- near_null: float32 [18, 16384], P(None, ('slab', 'sub')), may hold values from -48 to 48
- aggregates: int32 [16384], P(('slab', 'sub')), may hold values from 0 to 63
- diag_block: float32 [9, 16384], P(None, ('slab', 'sub')), may hold values from -1 to 12, as said below
- off_blocks: float32 [26, 9, 16384], P(None, None, ('slab', 'sub')), may hold values from -18 to 18
- columns: int32 [26, 16384], P(None, ('slab', 'sub')), may hold values from 0 to 767, as said below
- sends: int32 [4, 2048], P(None, ('slab', 'sub')), may hold values from 0 to 511
- start_vector: float32 [3, 16384], P(None, ('slab', 'sub')), may hold values from -18 to 18
Outputs:
- prolong_off: bfloat16 [26, 18, 16384], P(None, None, ('slab', 'sub'))
- prolong_self: bfloat16 [18, 16384], P(None, ('slab', 'sub'))
- rho: float32 [], replicated
The draws below stay inside these ranges and needn't reach their ends.
Inputs may be any that keep to these rules, and one draw needn't show every extreme that they name: `diag_block`: each block, read as 3x3 row-major, is symmetric with diagonal entries between 6 and 12 and off-diagonal entries between -1 and 1. `columns`: entries below 512 name a node of the same device; an entry c of 512 or more names ghost slot c - 512. Row e lists, for each device, the local rows it sends to its neighbour at sub + 1, sub - 1, slab + 1, slab - 1 for e = 0, 1, 2, 3. `aggregates`: aggregates lie within one device.
All inputs are finite; a program needn't handle non-finite values.
Results may differ from the reference program's by a relative error of at most 0.001.
Values sent between devices are 32-bit elements; how exact they have to be, the bound alone decides.
A program may use at most 64 MiB of HBM per device.

```python
import jax
import jax.numpy as jnp
from jax import lax

NB = 512
K = 26
ITERS = 8
GH = 64
AGG = 64
NODES = 16384
N_SLAB = 4
N_SUB = 8


def draw_diag_block(key, part):
    first_key, second_key = jax.random.split(key)
    middle = jax.random.uniform(first_key, (3, NODES), jnp.float32, 6.0, 12.0)
    side = jax.random.uniform(second_key, (3, NODES), jnp.float32, -1.0, 1.0)
    return jnp.stack([middle[0], side[0], side[1], side[0], middle[1], side[2], side[1], side[2], middle[2]])


def draw_start_vector(key, part):
    owner = (jnp.arange(NODES, dtype=jnp.int32) // NB).astype(jnp.float32)
    last_device = float(max(NODES // NB - 1, 1))
    base = jnp.clip(jax.random.normal(key, (3, NODES), jnp.float32), -6.0, 6.0)
    scale = 3.0 ** (owner / last_device)
    return base * scale[None, :]


def draw_columns(key, part):
    local_key, remote_key, pick_key = jax.random.split(jax.random.fold_in(key, 17), 3)
    nearby = jax.random.randint(local_key, (K, NODES), 0, NB, jnp.int32)
    remote = jax.random.randint(remote_key, (K, NODES), NB, NB + 4 * GH, jnp.int32)
    chooser = jax.random.randint(pick_key, (K, NODES), 0, 100, jnp.int32)
    result = jnp.where(chooser < 15, remote, nearby).astype(jnp.int32)
    result = result.at[0, 0].set(0)
    result = result.at[1, 0].set(NB + 4 * GH - 1)
    return result


def with_ends(drawn, own_key, smallest, top_value):
    place = [jax.random.randint(jax.random.fold_in(own_key, axis), (), 0, length) for axis, length in enumerate(drawn.shape)]
    main_axis = drawn.shape.index(max(drawn.shape))
    next_to = place[:main_axis] + [(place[main_axis] + 1) % drawn.shape[main_axis]] + place[main_axis + 1:]
    return drawn.at[tuple(place)].set(smallest).at[tuple(next_to)].set(top_value)


def levels(own_key, shape, pieces, smallest, largest):
    factor_of, own = 1.0, jax.random.fold_in(own_key, 6)
    for dim, parts in pieces:
        steps = jnp.exp(jax.random.uniform(jax.random.fold_in(own, dim), (parts,), jnp.float32, smallest / len(pieces), largest / len(pieces)))
        factor_of = factor_of * jnp.repeat(steps, shape[dim] // parts).reshape([-1 if axis == dim else 1 for axis in range(len(shape))])
    return factor_of


def bell_draw(own_key, shape, width, most, cuts=(), held_as=jnp.bfloat16):
    drawn = width * jax.random.normal(own_key, shape, jnp.float32)
    if cuts:
        drawn = drawn * levels(own_key, shape, cuts, -0.22, 0.18)
    return jnp.clip(drawn, -most, most).astype(held_as)


def setup_inputs(seed: int = 0) -> dict:
    arg_keys = jax.random.split(jax.random.key(seed), 8)
    near_null = bell_draw(arg_keys[0], (18, NODES), 8.0, 48.0, ((1, 32),), jnp.float32)
    aggregates = with_ends(jax.random.randint(arg_keys[1], (NODES,), 0, AGG), jax.random.fold_in(arg_keys[1], 1), 0, AGG - 1).astype(jnp.int32)
    diag_block = draw_diag_block(jax.random.fold_in(arg_keys[7], 71), 0)
    off_blocks = bell_draw(arg_keys[3], (K, 9, NODES), 3.0, 18.0, ((2, 32),), jnp.float32)
    columns = draw_columns(jax.random.fold_in(arg_keys[7], 71), 0)
    sends = with_ends(jax.random.randint(arg_keys[5], (4, GH * N_SLAB * N_SUB), 0, NB), jax.random.fold_in(arg_keys[5], 1), 0, NB - 1).astype(jnp.int32)
    start_vector = draw_start_vector(jax.random.fold_in(arg_keys[7], 71), 0)
    return {"near_null": near_null, "aggregates": aggregates, "diag_block": diag_block, "off_blocks": off_blocks, "columns": columns, "sends": sends, "start_vector": start_vector}


OMEGA = 4.0 / 3.0
HIGHEST = lax.Precision.HIGHEST

def invert_blocks(diag_block):
    entries = [diag_block[position] for position in range(9)]
    cofactor = [entries[4] * entries[8] - entries[5] * entries[7], entries[5] * entries[6] - entries[3] * entries[8], entries[3] * entries[7] - entries[4] * entries[6], entries[2] * entries[7] - entries[1] * entries[8], entries[0] * entries[8] - entries[2] * entries[6], entries[1] * entries[6] - entries[0] * entries[7], entries[1] * entries[5] - entries[2] * entries[4], entries[2] * entries[3] - entries[0] * entries[5], entries[0] * entries[4] - entries[1] * entries[3]]
    determinant = entries[0] * cofactor[0] + entries[1] * cofactor[1] + entries[2] * cofactor[2]
    inverse = [cofactor[column * 3 + row_index] / determinant for row_index in range(3) for column in range(3)]
    return jnp.stack(inverse).reshape((3, 3) + diag_block.shape[1:])

def reference(near_null, aggregates, diag_block, off_blocks, columns, sends, start_vector):
    device_count = N_SLAB * N_SUB
    ghost_count = NB // 8
    group_count = NB // 8
    node_number = jnp.arange(NODES, dtype=jnp.int32)
    owner = (node_number // NB).astype(jnp.int32)
    segment = owner * group_count + aggregates
    counts = jax.ops.segment_sum(jnp.ones((NODES,), jnp.float32), segment, num_segments=device_count * group_count)
    tentative = near_null * lax.rsqrt(counts[segment])[None, :]
    inverse = invert_blocks(diag_block)
    device_number = jnp.arange(device_count, dtype=jnp.int32)
    slab_index = device_number // N_SUB
    sub_index = device_number % N_SUB
    neighbours = [(slab_index, sub_index - 1), (slab_index, sub_index + 1), (slab_index - 1, sub_index), (slab_index + 1, sub_index)]
    send_rows = sends.reshape(4, device_count, ghost_count)
    tables = []
    valids = []
    for direction in range(4):
        slab_pos, sub_pos = neighbours[direction]
        present = (slab_pos >= 0) & (slab_pos < N_SLAB) & (sub_pos >= 0) & (sub_pos < N_SUB)
        sender = (jnp.clip(slab_pos, 0, N_SLAB - 1) * N_SUB + jnp.clip(sub_pos, 0, N_SUB - 1)).astype(jnp.int32)
        tables.append(sender[:, None] * NB + send_rows[direction][sender])
        valids.append(jnp.broadcast_to(present[:, None], (device_count, ghost_count)))
    table = jnp.concatenate(tables, axis=1).reshape(-1).astype(jnp.int32)
    valid = jnp.concatenate(valids, axis=1).reshape(-1)
    inside = columns < NB
    remote_slot = jnp.clip(columns - NB, 0, 4 * ghost_count - 1)
    flat_slot = (owner[None, :] * (4 * ghost_count) + remote_slot).astype(jnp.int32)
    source = jnp.where(inside, owner[None, :] * NB + columns, table[flat_slot]).astype(jnp.int32)
    weight = jnp.where(inside, True, valid[flat_slot]).astype(jnp.float32)
    mats = off_blocks.reshape(off_blocks.shape[0], 3, 3, NODES)

    def operator(field):

        def add_slot(total, slot_data):
            block, anchor, scale = slot_data
            picked = field[:, anchor] * scale[None, :]
            return (total + jnp.einsum('rcn,cmn->rmn', block, picked.reshape(3, 1, NODES), precision=HIGHEST), None)
        total, unused = lax.scan(add_slot, jnp.zeros((3, 1, NODES), jnp.float32), (mats, source, weight))
        return field + jnp.einsum('rcn,cmn->rmn', inverse, total, precision=HIGHEST).reshape(3, NODES)
    earlier = start_vector
    current = start_vector
    for iteration in range(ITERS):
        earlier = current
        current = operator(current)
    rho = jnp.sqrt(jnp.sum(current * current) / (jnp.sum(earlier * earlier) + 1e-05))

    def slot_blocks(slot_data):
        block, anchor, scale = slot_data
        picked = (tentative[:, anchor] * scale[None, :]).reshape(3, 6, NODES)
        product = jnp.einsum('rcn,cmn->rmn', block, picked, precision=HIGHEST)
        scaled = jnp.einsum('rcn,cmn->rmn', inverse, product, precision=HIGHEST)
        return (-(OMEGA / rho) * scaled).reshape(18, NODES).astype(jnp.bfloat16)
    prolong_off = lax.map(slot_blocks, (mats, source, weight))
    prolong_self = ((1.0 - OMEGA / rho) * tentative).astype(jnp.bfloat16)
    return (prolong_off, prolong_self, rho)
```

```python
import functools

import jax
import jax.numpy as jnp
from jax import lax
from jax.experimental import pallas as pl
from jax.experimental.pallas import tpu as pltpu
from jax.sharding import PartitionSpec as P

ITERS = 8
OMEGA = 4.0 / 3.0
LANES = 128
MESH = pl.DeviceIdType.MESH


def lane_gather(table, lanes):
    return jnp.take_along_axis(table, lanes, axis=1, mode="promise_in_bounds")


def tile(number):
    return pl.ds(number * LANES, LANES)


def pick(tables, index, first):
    high = index >> 7
    low = index & (LANES - 1)
    out = jnp.zeros(index.shape, jnp.float32)
    for step, table in enumerate(tables):
        out = jnp.where(high == first + step, lane_gather(table, low), out)
    return out


def invert_rows(entries):
    cofactor = [
        entries[4] * entries[8] - entries[5] * entries[7],
        entries[5] * entries[6] - entries[3] * entries[8],
        entries[3] * entries[7] - entries[4] * entries[6],
        entries[2] * entries[7] - entries[1] * entries[8],
        entries[0] * entries[8] - entries[2] * entries[6],
        entries[1] * entries[6] - entries[0] * entries[7],
        entries[1] * entries[5] - entries[2] * entries[4],
        entries[2] * entries[3] - entries[0] * entries[5],
        entries[0] * entries[4] - entries[1] * entries[3],
    ]
    determinant = entries[0] * cofactor[0] + entries[1] * cofactor[1] + entries[2] * cofactor[2]
    return [
        cofactor[column * 3 + row] / determinant for row in range(3) for column in range(3)
    ]


def kernel(
    n_slab, n_sub,
    near_ref, agg_ref, diag_ref, off_hbm, cols_ref, sends_ref, start_ref,
    raw_ref, tent_ref, rho_ref,
    off_v, cols_p, cols_k, mats, dinv, text, hist, sidx,
    sendw, recvw, sendt, recvt, stat_a, stats_a, stat_b, stats_b,
    off_sem, sendw_sem, recvw_sem, sendt_sem, recvt_sem,
    sa_sem, ra_sem, sb_sem, rb_sem,
):
    slots, rows = cols_ref.shape
    half = sends_ref.shape[1]
    tiles = rows // LANES
    ktiles = cols_p.shape[0] // 8
    modes = near_ref.shape[0] // 3
    groups = rows // 8
    a = lax.axis_index("slab")
    b = lax.axis_index("sub")
    load = pltpu.make_async_copy(off_hbm, off_v.at[pl.ds(0, slots)], off_sem)
    load.start()

    recvw[...] = jnp.zeros_like(recvw)
    recvt[...] = jnp.zeros_like(recvt)
    barrier = pltpu.get_barrier_semaphore()
    for step in range(1, n_sub):
        pl.semaphore_signal(
            barrier, inc=1, device_id={"sub": lax.rem(b + step, n_sub)}, device_id_type=MESH
        )
    for step in range(1, n_slab):
        pl.semaphore_signal(
            barrier, inc=1, device_id={"slab": lax.rem(a + step, n_slab)}, device_id_type=MESH
        )

    ways = (
        ("sub", b + 1, 0, b < n_sub - 1, b > 0),
        ("sub", b - 1, 0, b > 0, b < n_sub - 1),
        ("slab", a + 1, 1, a < n_slab - 1, a > 0),
        ("slab", a - 1, 1, a > 0, a < n_slab - 1),
    )

    def w_copy(t, way):
        axis, target, pair, unused, unused2 = ways[way]
        return pltpu.make_async_remote_copy(
            src_ref=sendw.at[t, pair], dst_ref=recvw.at[t, way],
            send_sem=sendw_sem.at[t, way], recv_sem=recvw_sem.at[t, way],
            device_id={axis: target}, device_id_type=MESH,
        )

    def t_copy(way):
        axis, target, pair, unused, unused2 = ways[way]
        return pltpu.make_async_remote_copy(
            src_ref=sendt.at[pair], dst_ref=recvt.at[way],
            send_sem=sendt_sem.at[way], recv_sem=recvt_sem.at[way],
            device_id={axis: target}, device_id_type=MESH,
        )

    def each_target(make, act):
        for way in range(4):
            pl.when(ways[way][3])(functools.partial(act, make, way))

    def each_source(make):
        for way in range(4):
            pl.when(ways[way][4])(functools.partial(lambda way: make(way).wait_recv(), way))

    hist[...] = jnp.zeros_like(hist)
    hist[0, 0:3, :] = start_ref[...]
    for pair in range(2):
        sidx[pair] = jnp.broadcast_to(
            jnp.concatenate(
                [sends_ref[2 * pair : 2 * pair + 1, :], sends_ref[2 * pair + 1 : 2 * pair + 2, :]],
                axis=1,
            ),
            (8, LANES),
        )

    def pack_w(t):
        tables = [hist[t, :, tile(j)] for j in range(tiles)]
        for pair in range(2):
            sendw[t, pair] = pick(tables, sidx[pair], 0)

    pack_w(0)
    pl.semaphore_wait(barrier, n_sub - 1 + n_slab - 1)
    each_target(functools.partial(w_copy, 0), lambda make, way: make(way).start())

    agg = agg_ref[...]
    member = (
        jnp.broadcast_to(agg, (groups, rows)) == lax.broadcasted_iota(jnp.int32, (groups, rows), 0)
    ).astype(jnp.float32)
    counts = jnp.sum(member, axis=1, keepdims=True)
    sizes = jnp.sum(member * counts, axis=0, keepdims=True)
    tent = near_ref[...] * lax.rsqrt(sizes)
    tent_ref[...] = tent
    text[...] = jnp.zeros_like(text)
    for c in range(3):
        text[8 * c : 8 * c + modes, 0:rows] = tent_ref[modes * c : modes * (c + 1), :]
    for pair in range(2):
        for c in range(3):
            sendt[pair, 8 * c : 8 * c + 8, :] = pick(
                [text[8 * c : 8 * c + 8, tile(j)] for j in range(tiles)], sidx[pair], 0
            )
    each_target(t_copy, lambda make, way: make(way).start())

    cols_p[...] = jnp.zeros_like(cols_p)
    cols_p[0:slots, :] = cols_ref[...]
    for k in range(slots):
        cols_k[k] = cols_ref[k : k + 1, :]

    inverse = invert_rows([diag_ref[p : p + 1, :] for p in range(9)])
    for p in range(9):
        dinv[p : p + 1, :] = inverse[p]
    for k in range(slots, off_v.shape[0]):
        off_v[k] = jnp.zeros(off_v.shape[1:], jnp.float32)
    load.wait()
    for kt in range(ktiles):
        for j in range(tiles):
            block = [off_v[8 * kt : 8 * kt + 8, p, tile(j)] for p in range(9)]
            for r in range(3):
                scale = [
                    jnp.broadcast_to(dinv[3 * r + q : 3 * r + q + 1, tile(j)], (8, LANES))
                    for q in range(3)
                ]
                for c in range(3):
                    mats[3 * r + c, 8 * kt : 8 * kt + 8, tile(j)] = (
                        scale[0] * block[c] + scale[1] * block[3 + c] + scale[2] * block[6 + c]
                    )

    left = lax.broadcasted_iota(jnp.int32, (8, LANES), 1) < half
    per = -(-slots // (ITERS - 1))

    def slot_products(k, unused):
        for j in range(tiles):
            index = jnp.broadcast_to(cols_k[k, :, tile(j)], (8, LANES))
            picked = [
                pick([text[8 * c : 8 * c + 8, tile(i)] for i in range(tiles + 2)], index, 0)
                for c in range(3)
            ]

            def spread(p):
                return jnp.broadcast_to(off_v[k, p : p + 1, tile(j)], (8, LANES))

            product = [
                spread(3 * r) * picked[0]
                + spread(3 * r + 1) * picked[1]
                + spread(3 * r + 2) * picked[2]
                for r in range(3)
            ]
            for r in range(3):
                scaled = sum(
                    jnp.broadcast_to(dinv[3 * r + q : 3 * r + q + 1, tile(j)], (8, LANES))
                    * product[q]
                    for q in range(3)
                )
                raw_ref[k, modes * r : modes * (r + 1), tile(j)] = scaled[0:modes]
        return unused

    def contribute(tables, first, j, totals):
        for kt in range(ktiles):
            index = cols_p[8 * kt : 8 * kt + 8, tile(j)]
            for c in range(3):
                picked = pick(tables[c], index, first)
                for r in range(3):
                    term = mats[3 * r + c, 8 * kt : 8 * kt + 8, tile(j)] * picked
                    totals[r] = term if totals[r] is None else totals[r] + term
        return totals

    def iterate(t, unused):
        local = [
            [jnp.broadcast_to(hist[t, c : c + 1, tile(i)], (8, LANES)) for i in range(tiles)]
            for c in range(3)
        ]
        totals = [contribute(local, 0, j, [None] * 3) for j in range(tiles)]

        @pl.when(t == 1)
        def _():
            each_source(t_copy)
            for pair in range(2):
                for c in range(3):
                    text[8 * c : 8 * c + 8, tile(tiles + pair)] = jnp.where(
                        left,
                        recvt[2 * pair, 8 * c : 8 * c + 8, :],
                        recvt[2 * pair + 1, 8 * c : 8 * c + 8, :],
                    )

        lax.fori_loop(
            jnp.clip((t - 1) * per, 0, slots), jnp.clip(t * per, 0, slots), slot_products, 0
        )
        each_source(functools.partial(w_copy, t))
        merged = [jnp.where(left, recvw[t, 2 * pair], recvw[t, 2 * pair + 1]) for pair in range(2)]
        ghost = [
            [jnp.broadcast_to(merged[pair][c : c + 1], (8, LANES)) for pair in range(2)]
            for c in range(3)
        ]
        for j in range(tiles):
            total = contribute(ghost, tiles, j, totals[j])
            for r in range(3):
                hist[t + 1, r : r + 1, tile(j)] = hist[t, r : r + 1, tile(j)] + jnp.sum(
                    total[r], axis=0, keepdims=True
                )

        @pl.when(t < ITERS - 1)
        def _():
            pack_w(t + 1)
            each_target(functools.partial(w_copy, t + 1), lambda make, way: make(way).start())

        return unused

    lax.fori_loop(0, ITERS, iterate, 0)

    def squares(t):
        return jnp.sum(
            sum(hist[t, :, tile(j)] * hist[t, :, tile(j)] for j in range(tiles)),
            axis=0, keepdims=True,
        )

    row = lax.broadcasted_iota(jnp.int32, (8, LANES), 0)
    own = jnp.where(
        row == 0,
        jnp.broadcast_to(squares(ITERS), (8, LANES)),
        jnp.where(row == 1, jnp.broadcast_to(squares(ITERS - 1), (8, LANES)), 0.0),
    )

    def sum_along(value, axis, me, count, stat, stats, send_sem, recv_sem):
        stat[...] = value

        def to(step):
            return pltpu.make_async_remote_copy(
                src_ref=stat, dst_ref=stats.at[me],
                send_sem=send_sem.at[step], recv_sem=recv_sem.at[me],
                device_id={axis: lax.rem(me + step, count)}, device_id_type=MESH,
            )

        def come(step):
            source = lax.rem(me + step, count)
            return pltpu.make_async_remote_copy(
                src_ref=stat, dst_ref=stats.at[source],
                send_sem=send_sem.at[step], recv_sem=recv_sem.at[source],
                device_id={axis: source}, device_id_type=MESH,
            )

        for step in range(1, count):
            to(step).start()
        stats[me] = value
        for step in range(1, count):
            come(step).wait_recv()
        total = stats[0]
        for source in range(1, count):
            total = total + stats[source]
        for step in range(1, count):
            to(step).wait_send()
        return total

    part = sum_along(own, "sub", b, n_sub, stat_a, stats_a, sa_sem, ra_sem)
    whole = sum_along(part, "slab", a, n_slab, stat_b, stats_b, sb_sem, rb_sem)
    latest = jnp.sum(whole[0:1], axis=1, keepdims=True)
    previous = jnp.sum(whole[1:2], axis=1, keepdims=True)
    rho_ref[...] = jnp.sqrt(latest / (previous + 1e-05))

    each_target(t_copy, lambda make, way: make(way).wait_send())

    def drain(t, unused):
        each_target(functools.partial(w_copy, t), lambda make, way: make(way).wait_send())
        return unused

    lax.fori_loop(0, ITERS, drain, 0)


def body(n_slab, n_sub, near_null, aggregates, diag_block, off_blocks, columns, sends, start_vector):
    slots, nine, rows = off_blocks.shape
    padded = -(-slots // 8) * 8
    wide = rows + 2 * LANES
    f32 = jnp.float32
    vmem = pl.BlockSpec(memory_space=pltpu.VMEM)
    dma = pltpu.SemaphoreType.DMA
    raw, tentative, rho = pl.pallas_call(
        functools.partial(kernel, n_slab, n_sub),
        out_shape=(
            jax.ShapeDtypeStruct((slots, near_null.shape[0], rows), f32),
            jax.ShapeDtypeStruct(near_null.shape, f32),
            jax.ShapeDtypeStruct((1, 1), f32),
        ),
        in_specs=[vmem, vmem, vmem, pl.BlockSpec(memory_space=pl.ANY), vmem, vmem, vmem],
        out_specs=(vmem, vmem, vmem),
        scratch_shapes=[
            pltpu.VMEM((padded, nine, rows), f32),
            pltpu.VMEM((padded, rows), jnp.int32),
            pltpu.VMEM((slots, 1, rows), jnp.int32),
            pltpu.VMEM((9, padded, rows), f32),
            pltpu.VMEM((16, rows), f32),
            pltpu.VMEM((24, wide), f32),
            pltpu.VMEM((ITERS + 1, 8, rows), f32),
            pltpu.VMEM((2, 8, LANES), jnp.int32),
            pltpu.VMEM((ITERS, 2, 8, LANES), f32),
            pltpu.VMEM((ITERS, 4, 8, LANES), f32),
            pltpu.VMEM((2, 24, LANES), f32),
            pltpu.VMEM((4, 24, LANES), f32),
            pltpu.VMEM((8, LANES), f32),
            pltpu.VMEM((n_sub, 8, LANES), f32),
            pltpu.VMEM((8, LANES), f32),
            pltpu.VMEM((n_slab, 8, LANES), f32),
            dma,
            dma((ITERS, 4)),
            dma((ITERS, 4)),
            dma((4,)),
            dma((4,)),
            dma((n_sub,)),
            dma((n_sub,)),
            dma((n_slab,)),
            dma((n_slab,)),
        ],
        compiler_params=pltpu.CompilerParams(collective_id=0, has_side_effects=True),
        name="smooth",
    )(near_null, aggregates.reshape(1, rows), diag_block, off_blocks, columns, sends, start_vector)
    rho = rho.reshape(())
    factor = -(OMEGA / rho)
    prolong_off = (factor * raw).astype(jnp.bfloat16)
    prolong_self = ((1.0 - OMEGA / rho) * tentative).astype(jnp.bfloat16)
    return (prolong_off, prolong_self, rho)


def solution(mesh):
    placed = (
        P(None, ("slab", "sub")),
        P(("slab", "sub")),
        P(None, ("slab", "sub")),
        P(None, None, ("slab", "sub")),
        P(None, ("slab", "sub")),
        P(None, ("slab", "sub")),
        P(None, ("slab", "sub")),
    )
    return jax.shard_map(
        functools.partial(body, mesh.shape["slab"], mesh.shape["sub"]),
        mesh=mesh,
        in_specs=placed,
        out_specs=(P(None, None, ("slab", "sub")), P(None, ("slab", "sub")), P()),
        check_vma=False,
    )
```

```python
import functools

import jax
import jax.numpy as jnp
from jax import lax
from jax.experimental import pallas as pl
from jax.experimental.pallas import tpu as pltpu
from jax.sharding import PartitionSpec as P

ITERS = 8
OMEGA = 4.0 / 3.0
LANES = 128
MESH = pl.DeviceIdType.MESH


def lane_gather(table, lanes):
    return jnp.take_along_axis(table, lanes, axis=1, mode="promise_in_bounds")


def tile(number):
    return pl.ds(number * LANES, LANES)


def pick(tables, index, first):
    high = index >> 7
    low = index & (LANES - 1)
    out = jnp.zeros(index.shape, jnp.float32)
    for step, table in enumerate(tables):
        out = jnp.where(high == first + step, lane_gather(table, low), out)
    return out


def invert_rows(entries):
    cofactor = [
        entries[4] * entries[8] - entries[5] * entries[7],
        entries[5] * entries[6] - entries[3] * entries[8],
        entries[3] * entries[7] - entries[4] * entries[6],
        entries[2] * entries[7] - entries[1] * entries[8],
        entries[0] * entries[8] - entries[2] * entries[6],
        entries[1] * entries[6] - entries[0] * entries[7],
        entries[1] * entries[5] - entries[2] * entries[4],
        entries[2] * entries[3] - entries[0] * entries[5],
        entries[0] * entries[4] - entries[1] * entries[3],
    ]
    determinant = entries[0] * cofactor[0] + entries[1] * cofactor[1] + entries[2] * cofactor[2]
    return [
        cofactor[column * 3 + row] / determinant for row in range(3) for column in range(3)
    ]


def unit_places(slots, tiles):
    units = []
    for k in range(0, slots - 7, 8):
        for j in range(tiles):
            units.append([(0, k, 8, j)])
    rest = slots % 8
    if rest:
        share = 8 // rest
        for j in range(0, tiles, share):
            units.append(
                [
                    (rest * i, slots - rest, rest, j + i)
                    for i in range(min(share, tiles - j))
                ]
            )
    return units


def scale_kernel(raw_ref, tent_ref, rho_ref, off_ref, self_ref):
    slots, rows = off_ref.shape[1:]
    inverse = OMEGA / rho_ref[...]
    factor = jnp.broadcast_to(-inverse, (8, LANES))
    places = unit_places(slots, rows // LANES)
    for j in range(rows // LANES):
        for entry in range(off_ref.shape[0]):
            parts = [
                (raw_ref[entry, u] * factor)[at : at + count]
                for u in range(len(places))
                for at, k, count, tile_number in places[u]
                if tile_number == j
            ]
            off_ref[entry, :, tile(j)] = jnp.concatenate(parts, axis=0).astype(off_ref.dtype)
    self_ref[...] = ((1.0 - inverse) * tent_ref[...]).astype(self_ref.dtype)


def kernel(
    n_slab, n_sub,
    near_hbm, agg_hbm, diag_hbm, off_hbm, cols_hbm, sends_hbm, start_hbm,
    raw_hbm, tent_ref, rho_ref,
    near_ref, agg_ref, diag_ref, cols_ref, sends_ref, start_ref, raw_ref, off_v, cols_u, mats, dinv, text, hist, sidx,
    sendw, recvw, sendt, recvt, stat, stats,
    off_sem, raw_sem, sendw_sem, recvw_sem, sendt_sem, recvt_sem,
    ss_sem, rs_sem,
):
    slots, rows = cols_ref.shape
    half = sends_ref.shape[1]
    tiles = rows // LANES
    units = unit_places(slots, tiles)
    modes = near_ref.shape[0] // 3
    groups = rows // 8
    a = lax.axis_index("slab")
    b = lax.axis_index("sub")
    loads = [
        pltpu.make_async_copy(source, target, off_sem.at[number])
        for number, (source, target) in enumerate(
            (
                (start_hbm, start_ref),
                (sends_hbm, sends_ref),
                (agg_hbm, agg_ref),
                (near_hbm, near_ref),
                (diag_hbm, diag_ref),
                (cols_hbm, cols_ref),
                (off_hbm, off_v),
            )
        )
    ]
    for load in loads:
        load.start()

    recvw[...] = jnp.zeros_like(recvw)
    recvt[...] = jnp.zeros_like(recvt)
    barrier = pltpu.get_barrier_semaphore()

    def greet(step, unused):
        target = lax.rem(a * n_sub + b + step, n_slab * n_sub)
        pl.semaphore_signal(
            barrier, inc=1,
            device_id={"slab": lax.div(target, n_sub), "sub": lax.rem(target, n_sub)},
            device_id_type=MESH,
        )
        return unused

    lax.fori_loop(1, n_slab * n_sub, greet, 0)

    ways = (
        ("sub", b + 1, 0, b < n_sub - 1, b > 0),
        ("sub", b - 1, 0, b > 0, b < n_sub - 1),
        ("slab", a + 1, 1, a < n_slab - 1, a > 0),
        ("slab", a - 1, 1, a > 0, a < n_slab - 1),
    )

    def w_copy(t, way):
        axis, target, pair, unused, unused2 = ways[way]
        return pltpu.make_async_remote_copy(
            src_ref=sendw.at[t, pair], dst_ref=recvw.at[t, way],
            send_sem=sendw_sem.at[t, way], recv_sem=recvw_sem.at[t, way],
            device_id={axis: target}, device_id_type=MESH,
        )

    def t_copy(way):
        axis, target, pair, unused, unused2 = ways[way]
        return pltpu.make_async_remote_copy(
            src_ref=sendt.at[pair], dst_ref=recvt.at[way],
            send_sem=sendt_sem.at[way], recv_sem=recvt_sem.at[way],
            device_id={axis: target}, device_id_type=MESH,
        )

    def each_target(make, act):
        for way in range(4):
            pl.when(ways[way][3])(functools.partial(act, make, way))

    def each_source(make):
        for way in range(4):
            pl.when(ways[way][4])(functools.partial(lambda way: make(way).wait_recv(), way))

    hist[...] = jnp.zeros_like(hist)
    loads[0].wait()
    loads[1].wait()
    hist[0, 0:3, :] = start_ref[...]
    for pair in range(2):
        sidx[pair] = jnp.broadcast_to(
            jnp.concatenate(
                [sends_ref[2 * pair : 2 * pair + 1, :], sends_ref[2 * pair + 1 : 2 * pair + 2, :]],
                axis=1,
            ),
            (8, LANES),
        )

    def pack_w(t):
        tables = [hist[t, :, tile(j)] for j in range(tiles)]
        for pair in range(2):
            sendw[t, pair] = pick(tables, sidx[pair], 0)[0:4]

    pack_w(0)

    loads[2].wait()
    loads[3].wait()
    agg = agg_ref[...]
    member = (
        jnp.broadcast_to(agg, (groups, rows)) == lax.broadcasted_iota(jnp.int32, (groups, rows), 0)
    ).astype(jnp.float32)
    counts = jnp.sum(member, axis=1, keepdims=True)
    sizes = jnp.sum(member * counts, axis=0, keepdims=True)
    tent = near_ref[...] * lax.rsqrt(sizes)
    tent_ref[...] = tent
    text[...] = jnp.zeros_like(text)
    for c in range(3):
        text[8 * c : 8 * c + modes, 0:rows] = tent_ref[modes * c : modes * (c + 1), :]
    for pair in range(2):
        for c in range(3):
            sendt[pair, 8 * c : 8 * c + 8, :] = pick(
                [text[8 * c : 8 * c + 8, tile(j)] for j in range(tiles)], sidx[pair], 0
            )

    loads[4].wait()
    loads[5].wait()
    for u, places in enumerate(units):
        if len(places) * places[0][2] < 8:
            cols_u[u] = jnp.zeros((8, LANES), jnp.int32)
        for at, k, count, j in places:
            cols_u[u, at : at + count, :] = cols_ref[k : k + count, tile(j)]

    inverse = invert_rows([diag_ref[p : p + 1, :] for p in range(9)])
    for p in range(9):
        dinv[p : p + 1, :] = inverse[p]
    pl.semaphore_wait(barrier, n_slab * n_sub - 1)
    each_target(functools.partial(w_copy, 0), lambda make, way: make(way).start())
    each_target(t_copy, lambda make, way: make(way).start())
    loads[6].wait()
    for u, places in enumerate(units):
        if len(places) * places[0][2] < 8:
            mats[u] = jnp.zeros(mats.shape[1:], jnp.float32)
        for at, k, count, j in places:
            block = [off_v[p, k : k + count, tile(j)] for p in range(9)]
            for r in range(3):
                scale = [
                    jnp.broadcast_to(dinv[3 * r + q : 3 * r + q + 1, tile(j)], (count, LANES))
                    for q in range(3)
                ]
                for c in range(3):
                    mats[u, 3 * r + c, at : at + count, :] = (
                        scale[0] * block[c] + scale[1] * block[3 + c] + scale[2] * block[6 + c]
                    )

    left = lax.broadcasted_iota(jnp.int32, (8, LANES), 1) < half
    per = -(-len(units) // (ITERS - 1))

    def unit_products(u, unused):
        index = cols_u[u]
        for m in range(modes):
            picked = [
                pick(
                    [
                        jnp.broadcast_to(text[8 * c + m : 8 * c + m + 1, tile(i)], (8, LANES))
                        for i in range(tiles + 2)
                    ],
                    index,
                    0,
                )
                for c in range(3)
            ]
            for r in range(3):
                raw_ref[modes * r + m, u] = (
                    mats[u, 3 * r] * picked[0]
                    + mats[u, 3 * r + 1] * picked[1]
                    + mats[u, 3 * r + 2] * picked[2]
                )
        return unused

    def contribute(tables, first, u):
        index = cols_u[u]
        picked = [pick(tables[c], index, first) for c in range(3)]
        return [sum(mats[u, 3 * r + c] * picked[c] for c in range(3)) for r in range(3)]

    def by_tile(terms):
        whole = [[None] * tiles for r in range(3)]
        for r in range(3):
            for u, places in enumerate(units):
                if len(places) == 1 and places[0][2] == 8:
                    j = places[0][3]
                    old = whole[r][j]
                    whole[r][j] = terms[u][r] if old is None else old + terms[u][r]
            for j in range(tiles):
                old = whole[r][j]
                whole[r][j] = 0.0 if old is None else jnp.sum(old, axis=0, keepdims=True)
            for u, places in enumerate(units):
                if not (len(places) == 1 and places[0][2] == 8):
                    for at, k, count, j in places:
                        whole[r][j] = whole[r][j] + jnp.sum(
                            terms[u][r][at : at + count], axis=0, keepdims=True
                        )
        return whole

    def iterate(t, unused):
        local = [
            [jnp.broadcast_to(hist[t, c : c + 1, tile(i)], (8, LANES)) for i in range(tiles)]
            for c in range(3)
        ]
        inner = by_tile([contribute(local, 0, u) for u in range(len(units))])
        for r in range(3):
            for j in range(tiles):
                hist[t + 1, r : r + 1, tile(j)] = hist[t, r : r + 1, tile(j)] + inner[r][j]

        @pl.when(t == 1)
        def _():
            each_source(t_copy)
            for pair in range(2):
                for c in range(3):
                    text[8 * c : 8 * c + 8, tile(tiles + pair)] = jnp.where(
                        left,
                        recvt[2 * pair, 8 * c : 8 * c + 8, :],
                        recvt[2 * pair + 1, 8 * c : 8 * c + 8, :],
                    )

        lax.fori_loop(
            jnp.clip((t - 1) * per, 0, len(units)), jnp.clip(t * per, 0, len(units)), unit_products, 0
        )
        each_source(functools.partial(w_copy, t))
        merged = [jnp.where(left[0:4], recvw[t, 2 * pair], recvw[t, 2 * pair + 1]) for pair in range(2)]
        ghost = [
            [jnp.broadcast_to(merged[pair][c : c + 1], (8, LANES)) for pair in range(2)]
            for c in range(3)
        ]
        outer = by_tile([contribute(ghost, tiles, u) for u in range(len(units))])
        for r in range(3):
            for j in range(tiles):
                hist[t + 1, r : r + 1, tile(j)] = hist[t + 1, r : r + 1, tile(j)] + outer[r][j]

        @pl.when(t < ITERS - 1)
        def _():
            pack_w(t + 1)
            each_target(functools.partial(w_copy, t + 1), lambda make, way: make(way).start())

        return unused

    lax.fori_loop(0, ITERS, iterate, 0)

    store = pltpu.make_async_copy(raw_ref, raw_hbm, raw_sem)
    store.start()

    def squares(t):
        return jnp.sum(
            sum(hist[t, :, tile(j)] * hist[t, :, tile(j)] for j in range(tiles)), keepdims=True
        )

    lane = lax.broadcasted_iota(jnp.int32, (1, LANES), 1)
    latest = jnp.broadcast_to(squares(ITERS), (1, LANES))
    previous = jnp.broadcast_to(squares(ITERS - 1), (1, LANES))
    own = jnp.where(lane == 0, latest, jnp.where(lane == 1, previous, 0.0))
    me = a * n_sub + b
    devices = n_slab * n_sub
    stat[0] = own

    def stat_copy(step, source):
        target = lax.rem(me + step, devices)
        landing = lax.rem(me + devices - step, devices) if source else me
        return pltpu.make_async_remote_copy(
            src_ref=stat.at[0], dst_ref=stats.at[landing],
            send_sem=ss_sem.at[step], recv_sem=rs_sem.at[landing],
            device_id={"slab": lax.div(target, n_sub), "sub": lax.rem(target, n_sub)},
            device_id_type=MESH,
        )

    def begin(step, unused):
        stat_copy(step, False).start()
        return unused

    def arrive(step, unused):
        stat_copy(step, True).wait_recv()
        return unused

    def sent(step, unused):
        stat_copy(step, False).wait_send()
        return unused

    lax.fori_loop(1, devices, begin, 0)
    stats[me] = own
    lax.fori_loop(1, devices, arrive, 0)
    whole = jnp.sum(stats[...], axis=0)
    latest = whole[:, 0:1]
    previous = whole[:, 1:2]
    rho_ref[...] = jnp.sqrt(latest / (previous + 1e-05))

    lax.fori_loop(1, devices, sent, 0)
    store.wait()
    each_target(t_copy, lambda make, way: make(way).wait_send())

    def drain(t, unused):
        each_target(functools.partial(w_copy, t), lambda make, way: make(way).wait_send())
        return unused

    lax.fori_loop(0, ITERS, drain, 0)


def body(n_slab, n_sub, near_null, aggregates, diag_block, off_blocks, columns, sends, start_vector):
    slots, nine, rows = off_blocks.shape
    wide = rows + 2 * LANES
    count = len(unit_places(slots, rows // LANES))
    f32 = jnp.float32
    vmem = pl.BlockSpec(memory_space=pltpu.VMEM)
    dma = pltpu.SemaphoreType.DMA
    raw, tentative, rho = pl.pallas_call(
        functools.partial(kernel, n_slab, n_sub),
        out_shape=(
            jax.ShapeDtypeStruct((near_null.shape[0], count, 8, LANES), f32),
            jax.ShapeDtypeStruct(near_null.shape, f32),
            jax.ShapeDtypeStruct((1, 1), f32),
        ),
        in_specs=[pl.BlockSpec(memory_space=pl.ANY)] * 7,
        out_specs=(pl.BlockSpec(memory_space=pl.ANY), vmem, vmem),
        scratch_shapes=[
            pltpu.VMEM(near_null.shape, f32),
            pltpu.VMEM((1, rows), jnp.int32),
            pltpu.VMEM(diag_block.shape, f32),
            pltpu.VMEM(columns.shape, jnp.int32),
            pltpu.VMEM(sends.shape, jnp.int32),
            pltpu.VMEM(start_vector.shape, f32),
            pltpu.VMEM((near_null.shape[0], count, 8, LANES), f32),
            pltpu.VMEM((nine, slots, rows), f32),
            pltpu.VMEM((count, 8, LANES), jnp.int32),
            pltpu.VMEM((count, nine, 8, LANES), f32),
            pltpu.VMEM((16, rows), f32),
            pltpu.VMEM((24, wide), f32),
            pltpu.VMEM((ITERS + 1, 8, rows), f32),
            pltpu.VMEM((2, 8, LANES), jnp.int32),
            pltpu.VMEM((ITERS, 2, 4, LANES), f32),
            pltpu.VMEM((ITERS, 4, 4, LANES), f32),
            pltpu.VMEM((2, 24, LANES), f32),
            pltpu.VMEM((4, 24, LANES), f32),
            pltpu.VMEM((1, 1, LANES), f32),
            pltpu.VMEM((n_slab * n_sub, 1, LANES), f32),
            dma((7,)),
            dma,
            dma((ITERS, 4)),
            dma((ITERS, 4)),
            dma((4,)),
            dma((4,)),
            dma((n_slab * n_sub,)),
            dma((n_slab * n_sub,)),
        ],
        compiler_params=pltpu.CompilerParams(collective_id=0, has_side_effects=True),
        name="smooth",
    )(
        near_null, aggregates.reshape(1, rows), diag_block, off_blocks.transpose(1, 0, 2),
        columns, sends, start_vector,
    )
    prolong_off, prolong_self = pl.pallas_call(
        scale_kernel,
        out_shape=(
            jax.ShapeDtypeStruct((near_null.shape[0], slots, rows), jnp.bfloat16),
            jax.ShapeDtypeStruct(near_null.shape, jnp.bfloat16),
        ),
        in_specs=[vmem, vmem, vmem],
        out_specs=(vmem, vmem),
        name="scale",
    )(raw, tentative, rho)
    return (prolong_off.transpose(1, 0, 2), prolong_self, rho.reshape(()))


def solution(mesh):
    placed = (
        P(None, ("slab", "sub")),
        P(("slab", "sub")),
        P(None, ("slab", "sub")),
        P(None, None, ("slab", "sub")),
        P(None, ("slab", "sub")),
        P(None, ("slab", "sub")),
        P(None, ("slab", "sub")),
    )
    return jax.shard_map(
        functools.partial(body, mesh.shape["slab"], mesh.shape["sub"]),
        mesh=mesh,
        in_specs=placed,
        out_specs=(P(None, None, ("slab", "sub")), P(None, ("slab", "sub")), P()),
        check_vma=False,
    )
```
